32 devices in a mesh: expert: 4 (over y, x), dp: 8 (over z, core).
Axes of the slice: x: 2, y: 2, z: 4, core: 2. Of those that a mesh axis runs over, the one named last changes fastest.
Arguments:
- acts: bfloat16 [32, 4, 16, 3584], P(('expert', 'dp')), may hold values from -6 to 6
- grad_out: bfloat16 [32, 4, 16, 1024], P(('expert', 'dp')), may hold values from -0.375 to 0.375
- routing_counts: int32 [32, 4], P(('expert', 'dp')), may hold values from 1 to 16, as said below
- left_basis: bfloat16 [4, 3584, 3584], P('expert', 'dp'), may hold values from -1 to 1, as said below
- right_basis: bfloat16 [4, 1024, 1024], P('expert'), may hold values from -1 to 1, as said below
- first_moment: float32 [4, 3584, 1024], P('expert', 'dp'), may hold values from -3 to 3
- second_moment: float32 [4, 3584, 1024], P('expert', 'dp'), may hold values from 0.05 to 2000
Outputs:
- step_delta: bfloat16 [4, 3584, 1024], P('expert', 'dp')
- first_out: float32 [4, 3584, 1024], P('expert', 'dp')
- second_out: float32 [4, 3584, 1024], P('expert', 'dp')
- expert_rms: float32 [4], P('expert')
The draws below stay inside these ranges and needn't reach their ends.
Inputs may be any that keep to these rules, and one draw needn't show every extreme that they name: Slot s of shard i for expert e carries a routed token when s < routing_counts[i, e]; the other slots hold leftover values that belong to no token. In every shard some expert has all 16 slots live. `left_basis`: each expert's block is an orthogonal matrix rounded to bfloat16. `right_basis`: each expert's block is an orthogonal matrix rounded to bfloat16.
All inputs are finite; a program needn't handle non-finite values.
Results may differ from the reference program's by a relative error of at most 0.013.
Values may be sent and summed in bfloat16 or wider, within the bound.
A program may use at most 64 MiB of HBM per device.

```python
import jax
import jax.numpy as jnp
from jax import lax

D = 3584
FF = 1024
CAP = 16
EXPERTS = 4
SHARDS = 32
N_EXPERT = 4
N_DP = 8


def orthogonal_blocks(base_key, block_count, order, diagonal_weight):

    def single(block_key):
        normal_block = jax.random.normal(block_key, (order, order), jnp.float32) / jnp.sqrt(jnp.float32(order))
        normal_block = normal_block + diagonal_weight * jnp.eye(order, dtype=jnp.float32)
        orthonormal, triangle = jnp.linalg.qr(normal_block)
        return orthonormal * jnp.sign(jnp.diagonal(triangle))[None, :]
    return lax.map(single, jax.random.split(base_key, block_count))


def draw_left_basis(key, part):
    return orthogonal_blocks(jax.random.fold_in(key, 11), EXPERTS, D, 1.5).astype(jnp.bfloat16)


def draw_right_basis(key, part):
    return orthogonal_blocks(jax.random.fold_in(key, 23), EXPERTS, FF, 0.0).astype(jnp.bfloat16)


def draw_second_moment(key, part):
    base_key = jax.random.fold_in(key, 37)
    log_low = jnp.log(jnp.float32(0.05))
    log_high = jnp.log(jnp.float32(2.0))
    base = jnp.exp(jax.random.uniform(base_key, (EXPERTS, D, FF), jnp.float32, log_low, log_high))
    row_span = 16.0
    expert_span = 9.0
    row_place = lax.broadcasted_iota(jnp.float32, (EXPERTS, D, FF), 1) / D
    expert_place = lax.broadcasted_iota(jnp.float32, (EXPERTS, D, FF), 0) / EXPERTS
    row_factor = jnp.exp((1.0 - row_place) * jnp.log(jnp.float32(row_span)))
    expert_factor = jnp.exp((1.0 - expert_place) * jnp.log(jnp.float32(expert_span)))
    return (base * row_factor * expert_factor).astype(jnp.float32)


def draw_routing_counts(key, part):
    first_key, second_key = jax.random.split(jax.random.fold_in(key, 5))
    counts = jax.random.randint(first_key, (SHARDS, EXPERTS), 1, CAP + 1)
    filled = jax.random.randint(second_key, (SHARDS, 1), 0, EXPERTS)
    column = lax.broadcasted_iota(jnp.int32, (SHARDS, EXPERTS), 1)
    return jnp.where(column == filled, CAP, counts).astype(jnp.int32)


def level_of(rng, shape, pieces, low, high):
    def one(position, parts):
        steps = jax.random.uniform(jax.random.fold_in(jax.random.fold_in(rng, 6), position), (parts,), jnp.float32, low / len(pieces), high / len(pieces))
        return jnp.repeat(jnp.exp(steps), shape[position] // parts).reshape((-1,) + (1,) * (len(shape) - position - 1))

    loudness = one(*pieces[0])
    for cut in pieces[1:]:
        loudness = loudness * one(*cut)
    return loudness


def centred(rng, extent, scale, bound, shards=(), held_as=jnp.bfloat16):
    values = jax.random.normal(rng, extent, jnp.float32) * scale
    if len(shards) > 0:
        values = level_of(rng, extent, shards, -0.22, 0.18) * values
    return jnp.clip(values, min=-bound, max=bound).astype(held_as)


def setup_inputs(seed: int = 0) -> dict:
    keys = jax.random.split(jax.random.key(seed), 8)
    return {
        "acts": centred(keys[0], (SHARDS, EXPERTS, CAP, D), 1.0, 6.0, ((0, 32),)),
        "grad_out": centred(keys[1], (SHARDS, EXPERTS, CAP, FF), (CAP * SHARDS // 2) ** -0.5, 0.375, ((0, 32),)),
        "routing_counts": draw_routing_counts(jax.random.fold_in(keys[7], 71), 0),
        "left_basis": draw_left_basis(jax.random.fold_in(keys[7], 71), 0),
        "right_basis": draw_right_basis(jax.random.fold_in(keys[7], 71), 0),
        "first_moment": centred(keys[5], (EXPERTS, D, FF), 0.5, 3.0, ((0, 4), (1, 8)), jnp.float32),
        "second_moment": draw_second_moment(jax.random.fold_in(keys[7], 71), 0),
    }


BETA_ONE = 0.9
BETA_TWO = 0.95
EPS_DIVIDE = 1e-08
EPS_MEAN = 1e-06

def reference(acts, grad_out, routing_counts, left_basis, right_basis, first_moment, second_moment):
    slot_index = lax.broadcasted_iota(jnp.int32, (SHARDS, EXPERTS, CAP), 2)
    live_slots = (slot_index < routing_counts[:, :, None])[..., None]
    acts_live = jnp.where(live_slots, acts, jnp.zeros((), jnp.bfloat16))
    grads_live = jnp.where(live_slots, grad_out, jnp.zeros((), jnp.bfloat16))
    acts_split = acts_live.reshape(N_EXPERT, N_DP, EXPERTS, CAP, D)
    grads_split = grads_live.reshape(N_EXPERT, N_DP, EXPERTS, CAP, FF)

    def one_expert(expert_index):
        token_acts = lax.dynamic_index_in_dim(acts_split, expert_index, 2, keepdims=False)
        token_grads = lax.dynamic_index_in_dim(grads_split, expert_index, 2, keepdims=False)
        token_acts = jnp.swapaxes(token_acts, 0, 1).reshape(N_DP, N_EXPERT * CAP, D)
        token_grads = jnp.swapaxes(token_grads, 0, 1).reshape(N_DP, N_EXPERT * CAP, FF)

        def add_partial(running, operand_pair):
            partial_value = jnp.dot(operand_pair[0].T.astype(jnp.float32), operand_pair[1].astype(jnp.float32), preferred_element_type=jnp.float32)
            partial_value = lax.optimization_barrier(partial_value.astype(jnp.bfloat16))
            return (running + partial_value.astype(jnp.float32), None)
        summed, _ = lax.scan(add_partial, jnp.zeros((D, FF), jnp.float32), (token_acts, token_grads))
        gradient = summed.astype(jnp.bfloat16)
        left_block = lax.dynamic_index_in_dim(left_basis, expert_index, 0, keepdims=False)
        right_block = lax.dynamic_index_in_dim(right_basis, expert_index, 0, keepdims=False)
        first_block = lax.dynamic_index_in_dim(first_moment, expert_index, 0, keepdims=False)
        second_block = lax.dynamic_index_in_dim(second_moment, expert_index, 0, keepdims=False)
        right_turned = jnp.dot(gradient.astype(jnp.float32), right_block.astype(jnp.float32), preferred_element_type=jnp.float32).astype(jnp.bfloat16)
        rotated = jnp.dot(left_block.T.astype(jnp.float32), right_turned.astype(jnp.float32), preferred_element_type=jnp.float32)
        first_new = BETA_ONE * first_block + (1.0 - BETA_ONE) * rotated
        second_new = BETA_TWO * second_block + (1.0 - BETA_TWO) * rotated * rotated
        direction = (first_new / (jnp.sqrt(second_new) + EPS_DIVIDE)).astype(jnp.bfloat16)
        restored = jnp.dot(direction.astype(jnp.float32), right_block.T.astype(jnp.float32), preferred_element_type=jnp.float32).astype(jnp.bfloat16)
        update = jnp.dot(left_block.astype(jnp.float32), restored.astype(jnp.float32), preferred_element_type=jnp.float32)
        squares = jnp.sum(update * update)
        return (update, first_new, second_new, squares)
    updates, first_out, second_out, squares = lax.map(one_expert, jnp.arange(EXPERTS, dtype=jnp.int32))
    expert_rms = jnp.sqrt(squares / (D * FF) + EPS_MEAN)
    mean_norm = jnp.mean(expert_rms)
    step_delta = (-updates / jnp.maximum(expert_rms, mean_norm)[:, None, None]).astype(jnp.bfloat16)
    return (step_delta, first_out, second_out, expert_rms)
```

```python
import functools

import jax
import jax.numpy as jnp
from jax import lax
from jax.experimental import pallas as pl
from jax.experimental.pallas import tpu as pltpu
from jax.sharding import PartitionSpec as P

BETA_ONE = 0.9
BETA_TWO = 0.95
EPS_DIVIDE = 1e-08
EPS_MEAN = 1e-06


def local(acts, grad_out, routing_counts, left_basis, right_basis, first_moment, second_moment):
    slot_count = acts.shape[2]
    slot_index = lax.broadcasted_iota(jnp.int32, routing_counts.shape + (slot_count,), 2)
    live_slots = (slot_index < routing_counts[:, :, None])[..., None]
    acts_live = jnp.where(live_slots, acts, jnp.zeros((), jnp.bfloat16))
    grads_live = jnp.where(live_slots, grad_out, jnp.zeros((), jnp.bfloat16))
    came_acts, came_grads = (
        lax.all_to_all(acts_live, "expert", split_axis=1, concat_axis=0, tiled=True),
        lax.all_to_all(grads_live, "expert", split_axis=1, concat_axis=0, tiled=True),
    )
    model_width = came_acts.shape[-1]
    hidden_width = came_grads.shape[-1]
    column_slabs = lax.all_to_all(came_acts, "dp", split_axis=3, concat_axis=0, tiled=True)
    grad_slabs = lax.all_gather(came_grads, "dp", axis=0, tiled=True)
    source_count = lax.axis_size("dp")
    column_slabs = column_slabs.reshape(source_count, -1, column_slabs.shape[-1])
    grad_slabs = grad_slabs.reshape(source_count, -1, hidden_width)
    partials = jnp.einsum(
        "stk,stf->skf", column_slabs, grad_slabs, preferred_element_type=jnp.float32
    )
    partials = lax.optimization_barrier(partials.astype(jnp.bfloat16))
    summed = jnp.sum(partials.astype(jnp.float32), axis=0)
    gradient = summed.astype(jnp.bfloat16)
    right_block = right_basis[0]
    left_rows = left_basis[0]
    right_turned = jnp.dot(gradient, right_block, preferred_element_type=jnp.float32).astype(
        jnp.bfloat16
    )
    basis_columns = left_rows
    rotated = lax.psum_scatter(
        jnp.einsum(
            "kc,kf->cf", basis_columns, right_turned, preferred_element_type=jnp.float32
        ).astype(jnp.bfloat16),
        "dp",
        scatter_dimension=0,
        tiled=True,
    ).astype(jnp.float32)
    first_new = BETA_ONE * first_moment[0] + (1.0 - BETA_ONE) * rotated
    second_new = BETA_TWO * second_moment[0] + (1.0 - BETA_TWO) * rotated * rotated
    direction = (first_new / (jnp.sqrt(second_new) + EPS_DIVIDE)).astype(jnp.bfloat16)
    restored = jnp.einsum(
        "kg,fg->kf", direction, right_block, preferred_element_type=jnp.float32
    ).astype(jnp.bfloat16)
    basis_columns = left_rows
    update = jnp.dot(
        basis_columns,
        lax.all_gather(restored, "dp", axis=0, tiled=True),
        preferred_element_type=jnp.float32,
    )
    squares = jnp.sum(update * update)
    cell_total = float(model_width * hidden_width)
    total_squares = lax.psum(squares, "dp")
    own_norm = jnp.sqrt(total_squares / cell_total + EPS_MEAN)
    norm_total = lax.psum(own_norm, "expert")
    mean_norm = norm_total / lax.axis_size("expert")
    step_delta = (-update / jnp.maximum(own_norm, mean_norm)).astype(jnp.bfloat16)
    return (step_delta[None], first_new[None], second_new[None], own_norm.reshape(1))


CORES = 2
PIECES = 2
TILE = 256
MESH = pl.DeviceIdType.MESH
VMEM_BYTES = 60 * 1024 * 1024


def remote(src, dst, send_sem, recv_sem, expert, dp):
    return pltpu.make_async_remote_copy(
        src_ref=src,
        dst_ref=dst,
        send_sem=send_sem,
        recv_sem=recv_sem,
        device_id=(expert, dp),
        device_id_type=MESH,
    )


def greet_all(experts, dps, expert, dp):
    barrier = pltpu.get_barrier_semaphore()
    for offset in range(1, experts * dps):
        target = (
            lax.rem(expert + offset // dps, experts),
            lax.rem(dp + offset % dps, dps),
        )
        pl.semaphore_signal(barrier, inc=1, device_id=target, device_id_type=MESH)
    pl.semaphore_wait(barrier, experts * dps - 1)


def exchange_kernel(
    experts, chips, acts, acts_out, acts_send, acts_recv, own_sem
):
    dps = chips * CORES
    expert, dp = lax.axis_index("expert"), lax.axis_index("dp")
    chip, core = dp // CORES, lax.rem(dp, CORES)
    greet_all(experts, dps, expert, dp)
    own_acts = pltpu.make_async_copy(
        acts.at[dp, expert], acts_out.at[core, expert, chip], own_sem
    )
    own_acts.start()
    acts_copies = []
    for chip_offset in reversed(range(chips)):
        to_chip = lax.rem(chip + chip_offset, chips)
        for expert_offset in range(experts):
            to_expert = lax.rem(expert + expert_offset, experts)
            for core_offset in range(CORES):
                if chip_offset + expert_offset + core_offset > 0:
                    to_dp = to_chip * CORES + lax.rem(core + core_offset, CORES)
                    index = (chip_offset * experts + expert_offset) * CORES + core_offset
                    copy = remote(
                        acts.at[to_dp, to_expert], acts_out.at[core, expert, chip],
                        acts_send.at[index], acts_recv.at[index], to_expert, to_dp,
                    )
                    copy.start()
                    acts_copies.append(copy)
    own_acts.wait()
    for copy in acts_copies:
        copy.wait()


def exchange(acts, experts, chips):
    slots, width = acts.shape[2:]
    count = experts * chips
    vmem = pl.BlockSpec(memory_space=pltpu.VMEM)
    dma = pltpu.SemaphoreType.DMA
    return pl.pallas_call(
        functools.partial(exchange_kernel, experts, chips),
        out_shape=jax.ShapeDtypeStruct((CORES, experts, chips, slots, width), acts.dtype),
        in_specs=[vmem],
        out_specs=vmem,
        scratch_shapes=[dma((count * CORES,)), dma((count * CORES,)), dma],
        compiler_params=pltpu.CompilerParams(
            collective_id=0, has_side_effects=True, vmem_limit_bytes=VMEM_BYTES
        ),
    )(acts)


def reduce_kernel(
    experts, chips, part, grads, out, grads_out, paired, held, came, total,
    pair_send, pair_recv, send_sem, recv_sem,
    grads_send, grads_recv, swap_send, swap_recv, own_sem,
):
    expert, dp = lax.axis_index("expert"), lax.axis_index("dp")
    chip, core = dp // CORES, lax.rem(dp, CORES)
    partner = chip * CORES + (1 - core)
    rows = out.shape[0]
    greet_all(experts, chips * CORES, expert, dp)

    def block(index):
        return part.at[pl.ds(pl.multiple_of(index * rows, 16), rows)]

    pairs = {}
    order = sorted(range(chips), key=lambda to: -abs(2 * to - chips + 1))
    for to in order:
        pairs[to] = remote(
            block(to * CORES + 1 - core), paired.at[to],
            pair_send.at[to], pair_recv.at[to], expert, partner,
        )
        pairs[to].start()

    own_grads = pltpu.make_async_copy(
        grads.at[expert], grads_out.at[core, expert, chip], own_sem
    )
    own_grads.start()
    grads_copies = []
    for chip_offset in reversed(range(chips)):
        to_chip = lax.rem(chip + chip_offset, chips)
        for expert_offset in range(experts):
            to_expert = lax.rem(expert + expert_offset, experts)
            if chip_offset + expert_offset > 0:
                index = chip_offset * experts + expert_offset
                copy = remote(
                    grads.at[to_expert], grads_out.at[core, expert, chip],
                    grads_send.at[index], grads_recv.at[index],
                    to_expert, to_chip * CORES + core,
                )
                copy.start()
                grads_copies.append(copy)

    def line_copy(way, to):
        step = CORES if way == 0 else -CORES
        return remote(
            held.at[to], came.at[way, to], send_sem.at[way, to], recv_sem.at[way, to],
            expert, dp + step,
        )

    def both(to):
        mine = block(to * CORES + core)[...].astype(jnp.float32)
        return mine + paired[to].astype(jnp.float32)

    def hand_on(way, to):
        first = (chip == 0) if way == 0 else (chip == chips - 1)
        before = (chip < to) if way == 0 else (chip > to)

        @pl.when(jnp.logical_and(before, first))
        def _():
            pairs[to].wait_recv()
            held[to] = both(to).astype(jnp.bfloat16)
            line_copy(way, to).start()

        @pl.when(jnp.logical_and(before, jnp.logical_not(first)))
        def _():
            pairs[to].wait_recv()
            value = both(to)
            came_sem = recv_sem.at[way, to]
            remote(
                came.at[way, to], came.at[way, to], send_sem.at[way, to], came_sem,
                expert, partner,
            ).wait_recv()
            held[to] = (value + came[way, to].astype(jnp.float32)).astype(jnp.bfloat16)
            line_copy(way, to).start()

    for step in range(chips - 1):
        hand_on(0, chips - 1 - step)
        hand_on(1, step)

    own_grads.wait()
    for copy in grads_copies:
        copy.wait_recv()
    swap = remote(
        grads_out.at[core], grads_out.at[core], swap_send, swap_recv, expert, partner
    )
    swap.start()
    remote(
        paired.at[chip], paired.at[chip], pair_send.at[chip], pair_recv.at[chip],
        expert, partner,
    ).wait_recv()
    total[...] = both(chip)
    for way, has in ((0, chip > 0), (1, chip < chips - 1)):

        @pl.when(has)
        def _(way=way):
            remote(
                came.at[way, chip], came.at[way, chip], send_sem.at[way, chip],
                recv_sem.at[way, chip], expert, partner,
            ).wait_recv()
            total[...] += came[way, chip].astype(jnp.float32)

    out[...] = total[...].astype(out.dtype)
    for copy in grads_copies:
        copy.wait_send()
    swap.wait()
    for to in range(chips):
        pairs[to].wait_send()

        @pl.when(chip < to)
        def _(to=to):
            line_copy(0, to).wait_send()

        @pl.when(chip > to)
        def _(to=to):
            line_copy(1, to).wait_send()


def reduce_rows(part, grads, experts, chips):
    rows, width = part.shape[0] // (chips * CORES), part.shape[1]
    vmem = pl.BlockSpec(memory_space=pltpu.VMEM)
    dma = pltpu.SemaphoreType.DMA
    return pl.pallas_call(
        functools.partial(reduce_kernel, experts, chips),
        out_shape=(
            jax.ShapeDtypeStruct((rows, width), part.dtype),
            jax.ShapeDtypeStruct((CORES, experts, chips) + grads.shape[1:], grads.dtype),
        ),
        in_specs=[vmem, vmem],
        out_specs=(vmem, vmem),
        scratch_shapes=[
            pltpu.VMEM((chips, rows, width), part.dtype),
            pltpu.VMEM((chips, rows, width), part.dtype),
            pltpu.VMEM((2, chips, rows, width), part.dtype),
            pltpu.VMEM((rows, width), jnp.float32),
            dma((chips,)), dma((chips,)), dma((2, chips)), dma((2, chips)),
            dma((experts * chips,)), dma((experts * chips,)), dma, dma, dma,
        ],
        compiler_params=pltpu.CompilerParams(
            collective_id=1, has_side_effects=True, vmem_limit_bytes=VMEM_BYTES
        ),
    )(part, grads)


def gather_kernel(
    experts, chips, mine, left, out, shared, held, squares,
    send_sem, recv_sem, pair_send, pair_recv, own_sem, share_send, share_recv,
):
    dps = chips * CORES
    expert, dp = lax.axis_index("expert"), lax.axis_index("dp")
    chip, core = dp // CORES, lax.rem(dp, CORES)
    partner = chip * CORES + (1 - core)
    rows, width = mine.shape
    piece_rows = rows // PIECES
    greet_all(experts, dps, expert, dp)

    def place(of, core_of, piece):
        start = (of * CORES + core_of) * rows + piece * piece_rows
        return held.at[pl.ds(pl.multiple_of(start, 16), piece_rows)]

    def part(piece):
        return mine.at[pl.ds(piece * piece_rows, piece_rows)]

    def line_copy(way, of, piece, src):
        step = CORES if way == 0 else -CORES
        return remote(
            src, place(of, core, piece), send_sem.at[way, of, piece],
            recv_sem.at[of, piece], expert, dp + step,
        )

    def pair_copy(of, piece, src):
        return remote(
            src, place(of, core, piece), pair_send.at[of, piece],
            pair_recv.at[of, piece], expert, partner,
        )

    for piece in range(PIECES):

        @pl.when(chip < chips - 1)
        def _():
            line_copy(0, chip, piece, part(piece)).start()

        @pl.when(chip > 0)
        def _():
            line_copy(1, chip, piece, part(piece)).start()

    own = pltpu.make_async_copy(
        mine, held.at[pl.ds(pl.multiple_of(dp * rows, 16), rows)], own_sem
    )
    own.start()
    for piece in range(PIECES):
        pair_copy(chip, piece, part(piece)).start()

    def multiply(of, begin):
        for piece in range(PIECES):
            remote(
                place(of, 1 - core, piece), place(of, 1 - core, piece),
                pair_send.at[of, piece], pair_recv.at[of, piece], expert, partner,
            ).wait_recv()
        depth = CORES * rows
        some = pl.ds(pl.multiple_of(of * depth, 128), depth)

        @pl.loop(0, width // TILE)
        def _(tile):
            columns = pl.ds(pl.multiple_of(tile * TILE, TILE), TILE)
            product = jnp.dot(
                left[:, some], held[some, columns], preferred_element_type=jnp.float32
            )
            if begin:
                out[:, columns] = product
            else:
                out[:, columns] += product

    def multiply_step(step):
        @pl.when(chip >= step)
        def _():
            multiply(chip - step, False)

        @pl.when(chip + step < chips)
        def _():
            multiply(chip + step, False)

    for step in range(1, chips):
        for piece in range(PIECES):
            for way in (0, 1):
                of = chip - step if way == 0 else chip + step
                there = (of >= 0) if way == 0 else (of < chips)
                goes_on = (chip < chips - 1) if way == 0 else (chip > 0)

                @pl.when(there)
                def _(of=of):
                    remote(
                        place(of, core, piece), place(of, core, piece),
                        pair_send.at[of, piece], recv_sem.at[of, piece], expert, partner,
                    ).wait_recv()

                @pl.when(jnp.logical_and(there, goes_on))
                def _(of=of, way=way):
                    line_copy(way, of, piece, place(of, core, piece)).start()

                @pl.when(there)
                def _(of=of):
                    pair_copy(of, piece, place(of, core, piece)).start()

            if piece == 0:
                if step == 1:
                    own.wait()
                    multiply(chip, True)
                else:
                    multiply_step(step - 1)
    multiply_step(chips - 1)
    value = out[...]
    squares[...] = jnp.full(squares.shape, jnp.sum(value * value), jnp.float32)
    copies = []
    for offset in range(1, experts * dps):
        copy = remote(
            squares, shared.at[expert, dp], share_send.at[offset], share_recv.at[offset],
            lax.rem(expert + offset // dps, experts), lax.rem(dp + offset % dps, dps),
        )
        copy.start()
        copies.append(copy)
    shared[expert, dp] = squares[...]
    for of in range(chips):
        for piece in range(PIECES):
            pair_copy(of, piece, place(of, core, piece)).wait_send()

            @pl.when(jnp.logical_and(chip >= of, chip < chips - 1))
            def _(of=of):
                line_copy(0, of, piece, place(of, core, piece)).wait_send()

            @pl.when(jnp.logical_and(chip <= of, chip > 0))
            def _(of=of):
                line_copy(1, of, piece, place(of, core, piece)).wait_send()

    for copy in copies:
        copy.wait()


def gather_multiply(mine, left, experts, chips):
    rows, width = mine.shape
    dps = chips * CORES
    vmem = pl.BlockSpec(memory_space=pltpu.VMEM)
    dma = pltpu.SemaphoreType.DMA
    return pl.pallas_call(
        functools.partial(gather_kernel, experts, chips),
        out_shape=(
            jax.ShapeDtypeStruct((rows, width), jnp.float32),
            jax.ShapeDtypeStruct((experts, dps, 8, 128), jnp.float32),
        ),
        in_specs=[vmem, vmem],
        out_specs=(vmem, vmem),
        scratch_shapes=[
            pltpu.VMEM((rows * dps, width), mine.dtype),
            pltpu.VMEM((8, 128), jnp.float32),
            dma((2, chips, PIECES)), dma((chips, PIECES)), dma((chips, PIECES)),
            dma((chips, PIECES)), dma, dma((experts * dps,)), dma((experts * dps,)),
        ],
        compiler_params=pltpu.CompilerParams(
            collective_id=2, has_side_effects=True, vmem_limit_bytes=VMEM_BYTES
        ),
    )(mine, left)


def local_tokens(
    experts, dps, acts, grad_out, routing_counts, left_basis, right_basis, first_moment, second_moment
):
    chips = dps // CORES
    slot_count = acts.shape[2]
    model_width, hidden_width = acts.shape[3], grad_out.shape[3]
    own_width = model_width // dps
    slot_index = lax.broadcasted_iota(jnp.int32, (experts, slot_count), 1)
    live_slots = (slot_index < routing_counts[0][:, None])[..., None]
    acts_live = jnp.where(live_slots, acts[0], jnp.zeros((), jnp.bfloat16))
    grads_live = jnp.where(live_slots, grad_out[0], jnp.zeros((), jnp.bfloat16))
    acts_cut = jnp.stack(
        [acts_live[:, :, i * own_width : (i + 1) * own_width] for i in range(dps)]
    )
    token_acts = exchange(acts_cut, experts, chips)
    token_acts = token_acts.reshape(-1, own_width)
    right_block = right_basis[0]
    left_rows = left_basis[0]
    turned_acts = jnp.einsum(
        "kc,tk->ct", left_rows, token_acts, preferred_element_type=jnp.float32
    ).astype(jnp.bfloat16)
    own_acts, token_grads = reduce_rows(turned_acts, grads_live, experts, chips)
    token_grads = token_grads.reshape(-1, hidden_width)
    turned_grads = jnp.dot(
        token_grads, right_block, preferred_element_type=jnp.float32
    ).astype(jnp.bfloat16)
    rotated = jnp.dot(own_acts, turned_grads, preferred_element_type=jnp.float32)
    first_new = BETA_ONE * first_moment[0] + (1.0 - BETA_ONE) * rotated
    second_new = BETA_TWO * second_moment[0] + (1.0 - BETA_TWO) * rotated * rotated
    direction = (first_new / (jnp.sqrt(second_new) + EPS_DIVIDE)).astype(jnp.bfloat16)
    restored = jnp.einsum(
        "kg,fg->kf", direction, right_block, preferred_element_type=jnp.float32
    ).astype(jnp.bfloat16)
    update, shared = gather_multiply(restored, left_rows, experts, chips)
    cell_total = float(model_width * hidden_width)
    norms = jnp.sqrt(jnp.sum(shared[:, :, 0, 0], axis=1) / cell_total + EPS_MEAN)
    own_norm = lax.dynamic_index_in_dim(norms, lax.axis_index("expert"), keepdims=False)
    mean_norm = jnp.mean(norms)
    step_delta = (-update / jnp.maximum(own_norm, mean_norm)).astype(jnp.bfloat16)
    return (step_delta[None], first_new[None], second_new[None], own_norm.reshape(1))


def pick(experts, dps, *args):
    acts, grad_out = args[0], args[1]
    tokens = acts.shape[2] * experts * dps
    rows = acts.shape[3] // dps
    small = tokens <= grad_out.shape[3] and dps % CORES == 0 and rows % (16 * PIECES) == 0
    small = small and CORES * rows % 128 == 0 and grad_out.shape[3] % TILE == 0
    if small and acts.shape[0] == 1 and acts.shape[1] == experts:
        return local_tokens(experts, dps, *args)
    return local(*args)


def solution(mesh):
    in_specs = (
        P(("expert", "dp"), None, None, None),
        P(("expert", "dp"), None, None, None),
        P(("expert", "dp"), None),
        P("expert", "dp", None),
        P("expert", None, None),
        P("expert", "dp", None),
        P("expert", "dp", None),
    )
    out_specs = (
        P("expert", "dp", None),
        P("expert", "dp", None),
        P("expert", "dp", None),
        P("expert"),
    )
    run = functools.partial(pick, mesh.shape["expert"], mesh.shape["dp"])
    return jax.shard_map(run, mesh=mesh, in_specs=in_specs, out_specs=out_specs, check_vma=False)
```
